32 devices in a mesh: spin: 1 (over z), row: 4 (over y), col: 8 (over x, core).
Axes of the slice: x: 4, y: 4, z: 1, core: 2. Of those that a mesh axis runs over, the one named last changes fastest.
The devices are a block of a 4x4x8 slice.
Arguments:
- hamiltonian: float32 [2304, 2304], P(('spin', 'row'), 'col')
- bounds: float32 [2], P('spin')
- n_occ: int32 [1], P('spin')
Outputs:
- output 1: float32 [2304, 2304], P(('spin', 'row'), 'col')
- output 2: float32 [1], P('spin')
All inputs are finite; a program needn't handle non-finite values.
Results may differ from the reference program's by a relative error of at most 0.001.
Values sent between devices are 32-bit elements.
A program may use at most 768 MiB of HBM per device.

```python
import jax
import jax.numpy as jnp
from jax import lax

N = 2304
STEPS = 3


def setup_inputs(seed: int = 0, part: int = 0) -> dict:
    key = jax.random.fold_in(jax.random.key(seed), part)
    k_off, k_diag, k_shift, k_margin, k_occ = jax.random.split(key, 5)
    gauss_mat = jax.random.normal(k_off, (N, N), jnp.float32)
    sym_part = (gauss_mat + gauss_mat.T) * (2.0 * N) ** -0.5
    unif_diag = jax.random.uniform(k_diag, (N,), jnp.float32)
    shift_val = 2.0 + jax.random.uniform(k_shift, (), jnp.float32)
    diag_vals = shift_val + 0.8 * (3.0 * unif_diag * unif_diag - 1.0)
    index_vec = jnp.arange(N)
    on_diag = index_vec[:, None] == index_vec[None, :]
    hamiltonian = jnp.where(on_diag, diag_vals[None, :], sym_part)
    margins = jax.random.uniform(k_margin, (2,), jnp.float32, 0.0, 0.5)
    bounds = jnp.stack([jnp.min(diag_vals) - 2.4 - margins[0], jnp.max(diag_vals) + 2.4 + margins[1]])
    n_occ = jax.random.randint(k_occ, (1,), 3 * N // 20, 7 * N // 20 + 1, jnp.int32)
    return {"hamiltonian": hamiltonian, "bounds": bounds, "n_occ": n_occ}


def reference(hamiltonian, bounds, n_occ):
    occupied = n_occ[0].astype(jnp.float32)
    mu_val = jnp.trace(hamiltonian) / N
    lam_scale = jnp.minimum(occupied / (bounds[1] - mu_val), (N - occupied) / (mu_val - bounds[0]))
    identity = jnp.eye(N, dtype=jnp.float32)
    density = (lam_scale / N) * (mu_val * identity - hamiltonian) + (occupied / N) * identity

    def purify_step(dens_cur, unused_x):
        dens_sq = jnp.dot(dens_cur, dens_cur, preferred_element_type=jnp.float32, precision=lax.Precision.HIGHEST)
        dens_cube = jnp.dot(dens_sq, dens_cur, preferred_element_type=jnp.float32, precision=lax.Precision.HIGHEST)
        trace_x = jnp.trace(dens_cur)
        trace_sq = jnp.sum(dens_cur * dens_cur)
        trace_cube = jnp.sum(dens_sq * dens_cur)
        mix_coef = (trace_sq - trace_cube) / (trace_x - trace_sq)
        updated = ((1.0 - 2.0 * mix_coef) * dens_cur + (1.0 + mix_coef) * dens_sq - dens_cube) / (1.0 - mix_coef)
        return updated, None

    density, _ = lax.scan(purify_step, density, None, length=STEPS)
    energy = 2.0 * jnp.sum(density * hamiltonian)
    return density, energy[None]
```

```python
import functools

import jax
import jax.numpy as jnp
from jax import lax
from jax.experimental import pallas as pl
from jax.experimental.pallas import tpu as pltpu
from jax.sharding import PartitionSpec as P

STEPS = 3
TILE = 256
LANES = 128
HIGHEST = lax.Precision.HIGHEST
MESH = pl.DeviceIdType.MESH

BACK1, FRONT1, OPP1, BACK2, FRONT2, OPP2, TWIN_OWN, TWIN_BACK, TWIN_FRONT, TWIN_OPP = range(10)


def dot_nn(a, b):
    return lax.dot_general(a, b, (((1,), (0,)), ((), ())), precision=HIGHEST, preferred_element_type=jnp.float32)


def dot_nt(a, b):
    return lax.dot_general(a, b, (((1,), (1,)), ((), ())), precision=HIGHEST, preferred_element_type=jnp.float32)


def total(v):
    return jnp.sum(jnp.sum(jnp.sum(v, axis=0), axis=0, keepdims=True), axis=1, keepdims=True)


def kernel(
    ny, nx, bounds_ref, occ_ref, ham_ref, dens_ref, energy_ref,
    store, slots, out_slots, out_blk, h_pan, x_pan, x2_pan, x3_pan, red,
    in_send, in_recv, out_send, out_recv, red_send, red_recv, g_send, g_recv,
):
    n_cols = 2 * nx
    n_dev = ny * n_cols
    rows_n, cols_n = ham_ref.shape
    order = cols_n * n_cols
    groups = order // TILE
    window = (groups + 1) // 2
    rpd = order // n_dev
    my_y = lax.axis_index("row")
    my_m = lax.axis_index("col")
    my_x, my_c = my_m // 2, lax.rem(my_m, 2)
    flat = store.reshape(2, window, 2, order, LANES)

    def dev(y, x, c):
        return {"row": y, "col": 2 * x + c}

    x_front, x_back, x_opp = (lax.rem(my_x + d + 2 * my_c, nx) for d in (1, 3, 2))
    x_opp = lax.rem(my_x + 2, nx)
    y_front, y_back = (lax.rem(my_y + d + 2 * my_c, ny) for d in (1, 3))
    y_opp = lax.rem(my_y + 2, ny)

    barrier = pltpu.get_barrier_semaphore()
    me = my_y * n_cols + my_m

    def sig(k, carry):
        t = lax.rem(me + k, n_dev)
        pl.semaphore_signal(barrier, inc=1, device_id={"row": t // n_cols, "col": lax.rem(t, n_cols)}, device_id_type=MESH)
        return carry

    lax.fori_loop(1, n_dev, sig, 0)

    row_id = my_y * rows_n + lax.broadcasted_iota(jnp.int32, (rows_n, cols_n), 0)
    col_id = my_m * cols_n + lax.broadcasted_iota(jnp.int32, (rows_n, cols_n), 1)
    tr_h = jnp.sum(jnp.sum(jnp.where(row_id == col_id, ham_ref[...], 0.0), axis=0, keepdims=True), axis=1, keepdims=True)
    lane = lax.broadcasted_iota(jnp.int32, (1, LANES), 1)

    def red_start(use, sums):
        row = jnp.zeros((1, LANES), jnp.float32)
        for q, s in enumerate(sums):
            row = jnp.where(lane == q, s, row)
        red[use, me] = row

        def push(k, carry):
            t = lax.rem(me + k, n_dev)
            pltpu.make_async_remote_copy(
                red.at[use, me], red.at[use, me], red_send.at[use], red_recv.at[use],
                device_id={"row": t // n_cols, "col": lax.rem(t, n_cols)}, device_id_type=MESH,
            ).start()
            return carry

        lax.fori_loop(1, n_dev, push, 0)

    def red_wait(use, count):
        many = red.at[use, pl.ds(0, n_dev - 1)]
        copy = pltpu.make_async_remote_copy(many, many, red_send.at[use], red_recv.at[use], device_id=dev(my_y, my_x, my_c), device_id_type=MESH)
        copy.wait_recv()
        copy.wait_send()
        row = jnp.sum(red[use], axis=0)
        return [jnp.sum(jnp.where(lane == q, row, 0.0), axis=1, keepdims=True) for q in range(count)]

    pl.semaphore_wait(barrier, n_dev - 1)
    red_start(0, [tr_h])

    def in_copy(m_to):
        r = pl.multiple_of(lax.rem(m_to, 2) * cols_n + (m_to // 2) * rpd, 8)
        return pltpu.make_async_remote_copy(
            ham_ref.at[pl.ds(r, rpd), :], slots.at[my_m], in_send.at[m_to], in_recv.at[my_m],
            device_id={"row": my_y, "col": m_to}, device_id_type=MESH,
        )

    def in_wait(m_from):
        return pltpu.make_async_remote_copy(
            slots.at[m_from], slots.at[m_from], in_send.at[m_from], in_recv.at[m_from],
            device_id={"row": my_y, "col": my_m}, device_id_type=MESH,
        )

    for k in range(1, n_cols):
        in_copy(lax.rem(my_m + k, n_cols)).start()
    slots[my_m] = ham_ref[pl.ds(pl.multiple_of(my_c * cols_n + my_x * rpd, 8), rpd), :]
    for k in range(1, n_cols):
        in_wait(lax.rem(my_m + k, n_cols)).wait_recv()

    panel = jnp.concatenate([slots[2 * (k % ny) + k // ny] for k in range(n_cols)], axis=1)
    for g in range(groups):
        h_pan[g] = panel[:, g * TILE:(g + 1) * TILE]

    first_row = rpd * (4 * (ny * my_c + my_y) + my_x)
    shape3 = (groups, rpd, TILE)
    diag = (first_row + lax.broadcasted_iota(jnp.int32, shape3, 1)) == (
        TILE * lax.broadcasted_iota(jnp.int32, shape3, 0) + lax.broadcasted_iota(jnp.int32, shape3, 2)
    )
    occupied = jnp.full((1, 1), occ_ref[0], jnp.int32).astype(jnp.float32)
    eps_min = jnp.full((1, 1), bounds_ref[0], jnp.float32)
    eps_max = jnp.full((1, 1), bounds_ref[1], jnp.float32)
    mu = red_wait(0, 1)[0] / order
    lam = jnp.minimum(occupied / (eps_max - mu), (order - occupied) / (mu - eps_min))
    x_pan[...] = jnp.where(diag, ((lam * mu + occupied) / order)[None], 0.0) - (lam / order)[None] * h_pan[...]

    group0 = first_row // TILE
    split = TILE * (group0 + 1) - first_row
    upper = lax.broadcasted_iota(jnp.int32, (rpd, TILE), 0) < split

    def step_body(step, carry):
        par = lax.rem(step, 2)

        def region(kind, chunk, half):
            at = store.at[par, chunk, half]
            if kind in (BACK1, FRONT1, OPP1, "own1"):
                x = {BACK1: x_back, FRONT1: x_front, OPP1: x_opp, "own1": my_x}[kind] if half == 0 else my_x
                y = {BACK1: y_back, FRONT1: y_front, OPP1: y_opp, "own1": my_y}[kind] if half == 1 else my_y
                return at.at[my_c, y, x]
            base = {TWIN_OWN: "own2", TWIN_BACK: BACK2, TWIN_FRONT: FRONT2, TWIN_OPP: OPP2}.get(kind, kind)
            if half == 0:
                return at.at[my_c, {BACK2: y_back, FRONT2: y_front, OPP2: y_opp, "own2": my_y}[base]]
            return at.at[my_c, :, {BACK2: x_back, FRONT2: x_front, OPP2: x_opp, "own2": my_x}[base]]

        def twin_region(kind, chunk, half):
            at = store.at[par, chunk, half]
            if half == 0:
                return at.at[1 - my_c, {TWIN_OWN: my_y, TWIN_BACK: y_front, TWIN_FRONT: y_back, TWIN_OPP: y_opp}[kind]]
            return at.at[1 - my_c, :, {TWIN_OWN: my_x, TWIN_BACK: x_front, TWIN_FRONT: x_back, TWIN_OPP: x_opp}[kind]]

        def target(kind, half):
            if kind >= TWIN_OWN:
                return dev(my_y, my_x, 1 - my_c)
            along_x = (half == 0) == (kind in (BACK1, FRONT1, OPP1))
            front = kind in (BACK1, OPP1, BACK2, OPP2)
            if along_x:
                return dev(my_y, x_front if front else x_back, my_c)
            return dev(y_front if front else y_back, my_x, my_c)

        def message(kind, chunk, half):
            src = region(
                {BACK1: "own1", FRONT1: "own1", OPP1: BACK1, BACK2: "own2", FRONT2: "own2", OPP2: BACK2}.get(kind, kind), chunk, half
            )
            hc = 2 * chunk + half
            return pltpu.make_async_remote_copy(
                src, src, g_send.at[hc, kind], g_recv.at[hc, kind], device_id=target(kind, half), device_id_type=MESH
            )

        def arrival(kind, chunk, half):
            dst = twin_region(kind, chunk, half) if kind >= TWIN_OWN else region(kind, chunk, half)
            hc = 2 * chunk + half
            return pltpu.make_async_remote_copy(
                dst, dst, g_send.at[hc, kind], g_recv.at[hc, kind], device_id=dev(my_y, my_x, my_c), device_id_type=MESH
            )

        def send(kind, chunk):
            for half in (0, 1):
                message(kind, chunk, half).start()

        def recv(kind, chunk):
            for half in (0, 1):
                arrival(kind, chunk, half).wait_recv()

        for chunk in range(window):
            piece = jnp.where(upper, x_pan[lax.rem(group0 + chunk, groups)], x_pan[lax.rem(group0 + 1 + chunk, groups)])
            for half in (0, 1):
                store[par, chunk, half, my_c, my_y, my_x] = piece[:, half * LANES:(half + 1) * LANES]
            send(BACK1, chunk)
            send(FRONT1, chunk)

        for g in range(groups):
            x2_pan[g] = jnp.zeros((rpd, TILE), jnp.float32)

        for chunk in range(window):
            recv(BACK1, chunk)
            send(OPP1, chunk)

        def spread(chunk):
            recv(FRONT1, chunk)
            recv(OPP1, chunk)
            send(BACK2, chunk)
            send(FRONT2, chunk)
            send(TWIN_OWN, chunk)

        def relay(chunk):
            recv(BACK2, chunk)
            send(OPP2, chunk)
            send(TWIN_BACK, chunk)

        def block(chunk, a):
            rows = pl.ds(pl.multiple_of(a * TILE, TILE), TILE)
            return jnp.concatenate([flat[par, chunk, 0, rows, :], flat[par, chunk, 1, rows, :]], axis=1)

        spread(0)
        spread(1)
        relay(0)
        for chunk in range(window):
            if chunk + 2 < window:
                spread(chunk + 2)
            if chunk + 1 < window:
                relay(chunk + 1)
            recv(FRONT2, chunk)
            send(TWIN_FRONT, chunk)
            recv(OPP2, chunk)
            send(TWIN_OPP, chunk)
            for kind in (TWIN_OWN, TWIN_BACK, TWIN_FRONT, TWIN_OPP):
                recv(kind, chunk)

            def gather_mul(a, carry, chunk=chunk):
                w = block(chunk, a)
                h = lax.rem(a + chunk, groups)
                x2_pan[h] += dot_nn(x_pan[a], w)
                if chunk:
                    x2_pan[a] += dot_nt(x_pan[h], w)
                return carry

            lax.fori_loop(0, groups, gather_mul, 0, unroll=3)

        x = x_pan[...]
        x2 = x2_pan[...]
        red_start(1 + step, [total(jnp.where(diag, x, 0.0)), total(x * x), total(x2 * x)])

        def cube(h, carry):
            acc = None
            for d in range(window):
                g = lax.rem(h + groups - d, groups)
                part = dot_nn(x2_pan[g], block(d, g))
                acc = part if acc is None else acc + part
            for d in range(1, window):
                acc = acc + dot_nt(x2_pan[lax.rem(h + d, groups)], block(d, h))
            x3_pan[h] = acc
            return carry

        lax.fori_loop(0, groups, cube, 0)

        t1, t2, t3 = red_wait(1 + step, 3)
        c = (t2 - t3) / (t1 - t2)
        x_pan[...] = ((1.0 - 2.0 * c)[None] * x_pan[...] + (1.0 + c)[None] * x2_pan[...] - x3_pan[...]) / (1.0 - c)[None]

        for chunk in range(window):
            for kind in range(10):
                for half in (0, 1):
                    message(kind, chunk, half).wait_send()
        return carry

    lax.fori_loop(0, STEPS, step_body, 0)

    red_start(1 + STEPS, [total(x_pan[...] * h_pan[...])])
    result = jnp.concatenate([x_pan[g] for g in range(groups)], axis=1)
    for k in range(n_cols):
        out_slots[2 * (k % ny) + k // ny] = result[:, k * cols_n:(k + 1) * cols_n]

    my_rows = pl.ds(pl.multiple_of(my_c * cols_n + my_x * rpd, 8), rpd)

    def out_copy(m_to):
        return pltpu.make_async_remote_copy(
            out_slots.at[m_to], out_blk.at[my_rows, :], out_send.at[m_to], out_recv.at[my_m],
            device_id={"row": my_y, "col": m_to}, device_id_type=MESH,
        )

    def out_wait(m_from):
        r = pl.ds(pl.multiple_of(lax.rem(m_from, 2) * cols_n + (m_from // 2) * rpd, 8), rpd)
        return pltpu.make_async_remote_copy(
            out_blk.at[r, :], out_blk.at[r, :], out_send.at[m_from], out_recv.at[m_from],
            device_id={"row": my_y, "col": my_m}, device_id_type=MESH,
        )

    for k in range(1, n_cols):
        out_copy(lax.rem(my_m + k, n_cols)).start()
    out_blk[my_rows, :] = out_slots[my_m]
    for k in range(1, n_cols):
        out_wait(lax.rem(my_m + k, n_cols)).wait_recv()
    dens_ref[...] = out_blk[...]
    energy_ref[...] = 2.0 * red_wait(1 + STEPS, 1)[0]
    for k in range(1, n_cols):
        in_copy(lax.rem(my_m + k, n_cols)).wait_send()
        out_copy(lax.rem(my_m + k, n_cols)).wait_send()


def solution(mesh):
    ny, n_cols = mesh.shape["row"], mesh.shape["col"]
    nx = n_cols // 2
    n_dev = ny * n_cols

    def local_fn(ham_blk, bounds, n_occ):
        rows_n, cols_n = ham_blk.shape
        order = cols_n * n_cols
        groups = order // TILE
        window = (groups + 1) // 2
        rpd = order // n_dev
        dens, energy = pl.pallas_call(
            functools.partial(kernel, ny, nx),
            out_shape=(jax.ShapeDtypeStruct((rows_n, cols_n), jnp.float32), jax.ShapeDtypeStruct((1, 1), jnp.float32)),
            in_specs=[pl.BlockSpec(memory_space=pltpu.SMEM)] * 2 + [pl.BlockSpec(memory_space=pltpu.VMEM)],
            out_specs=(pl.BlockSpec(memory_space=pltpu.VMEM),) * 2,
            scratch_shapes=[
                pltpu.VMEM((2, window, 2, 2, ny, nx, rpd, LANES), jnp.float32),
                pltpu.VMEM((n_cols, rpd, cols_n), jnp.float32),
                pltpu.VMEM((n_cols, rpd, cols_n), jnp.float32),
                pltpu.VMEM((rows_n, cols_n), jnp.float32),
                pltpu.VMEM((groups, rpd, TILE), jnp.float32),
                pltpu.VMEM((groups, rpd, TILE), jnp.float32),
                pltpu.VMEM((groups, rpd, TILE), jnp.float32),
                pltpu.VMEM((groups, rpd, TILE), jnp.float32),
                pltpu.VMEM((STEPS + 2, n_dev, 1, LANES), jnp.float32),
                pltpu.SemaphoreType.DMA((n_cols,)),
                pltpu.SemaphoreType.DMA((n_cols,)),
                pltpu.SemaphoreType.DMA((n_cols,)),
                pltpu.SemaphoreType.DMA((n_cols,)),
                pltpu.SemaphoreType.DMA((STEPS + 2,)),
                pltpu.SemaphoreType.DMA((STEPS + 2,)),
                pltpu.SemaphoreType.DMA((2 * window, 10)),
                pltpu.SemaphoreType.DMA((2 * window, 10)),
            ],
            compiler_params=pltpu.CompilerParams(collective_id=0, has_side_effects=True, vmem_limit_bytes=58 * 1024 * 1024),
            name="purify",
        )(bounds, n_occ, ham_blk)
        return dens, energy.reshape(1)

    spec_mat = P(("spin", "row"), "col")
    return jax.shard_map(local_fn, mesh=mesh, in_specs=(spec_mat, P("spin"), P("spin")), out_specs=(spec_mat, P("spin")), check_vma=False)
```
